32 devices in a mesh: row: 16 (over z, x, core), col: 2 (over y).
Axes of the slice: x: 2, y: 2, z: 4, core: 2. Of those that a mesh axis runs over, the one named last changes fastest.
Arguments:
- seq_state: bfloat16 [1024, 1024], P('row'), may hold values from -6 to 6
- pair_state: bfloat16 [1024, 1024, 128], P('row', 'col'), may hold values from -8 to 8
- w_bias: bfloat16 [128, 32], replicated, may hold values from -12 to 12
- w_qkv: bfloat16 [3, 1024, 1024], P(None, None, 'col'), may hold values from -0.1875 to 0.1875
- w_gate: bfloat16 [1024, 1024], P(None, 'col'), may hold values from -0.1875 to 0.1875
- w_out: bfloat16 [1024, 1024], replicated, may hold values from -0.8984375 to 0.8984375
- w_seq_pair: bfloat16 [1024, 128], replicated, may hold values from -0.1875 to 0.1875
- w_pair_out: bfloat16 [128, 128], replicated, may hold values from -0.5 to 0.5
- w_up: bfloat16 [128, 512], replicated, may hold values from -0.5 to 0.5
- w_down: bfloat16 [512, 128], replicated, may hold values from -0.25 to 0.25
Outputs:
- seq_out: bfloat16 [1024, 1024], P('row')
- pair_out: bfloat16 [1024, 1024, 128], P('row', 'col')
The draws below stay inside these ranges and needn't reach their ends.
All inputs are finite; a program needn't handle non-finite values.
Results may differ from the reference program's by a relative error of at most 0.018.
The reference program's roundings to bfloat16 on the way count: a program that leaves them out, or rounds other values in their place, can miss the bound.
Values may be sent and summed in bfloat16 or wider, within the bound.
A program may use at most 64 MiB of HBM per device.

```python
import math
import jax
import jax.numpy as jnp
from jax import lax

RES_DEV = 64
L = 1024
D = 1024
H = 32
P_SIZE = 128
INNER = 64
HID = 512


def draw_w_bias(key, part):
    base_draw = jnp.clip(jax.random.normal(jax.random.fold_in(key, 11), (P_SIZE, H), jnp.float32), -5.0, 5.0) * (2.0 / math.sqrt(P_SIZE))
    return base_draw.astype(jnp.bfloat16)


def draw_pair_state(key, part):
    values = jnp.clip(jax.random.normal(jax.random.fold_in(key, 23), (L, L, P_SIZE), jnp.float32), -6.0, 6.0)
    return values.astype(jnp.bfloat16)


def level_of(stream_key, extent, pieces, smallest, top_value):
    def one(axis_at, blocks):
        draws = jax.random.uniform(jax.random.fold_in(jax.random.fold_in(stream_key, 6), axis_at), (blocks,), jnp.float32, smallest / len(pieces), top_value / len(pieces))
        return jnp.repeat(jnp.exp(draws), extent[axis_at] // blocks).reshape((-1,) + (1,) * (len(extent) - axis_at - 1))

    level = one(*pieces[0])
    for cut in pieces[1:]:
        level = level * one(*cut)
    return level


def gaussian(key, dims, deviation, most, split=(), held_as=jnp.bfloat16):
    factor_of = level_of(key, dims, split, -0.22, 0.18) if split else 1.0
    values = jax.random.normal(key, dims, jnp.float32) * deviation * factor_of
    return jnp.minimum(jnp.maximum(values, -most), most).astype(held_as)


def setup_inputs(seed: int = 0) -> dict:
    arg_keys = jax.random.split(jax.random.key(seed), 11)
    seq_state = gaussian(arg_keys[0], (L, D), 1.0, 6.0, ((0, 16),))
    pair_state = draw_pair_state(jax.random.fold_in(arg_keys[10], 71), 0)
    w_bias = draw_w_bias(jax.random.fold_in(arg_keys[10], 71), 0)
    w_qkv = gaussian(arg_keys[3], (3, D, D), D ** -0.5, 0.1875, ((2, 2),))
    w_gate = gaussian(arg_keys[4], (D, D), D ** -0.5, 0.1875, ((1, 2),))
    w_out = gaussian(arg_keys[5], (D, D), 0.15, 0.8984375)
    w_seq_pair = gaussian(arg_keys[6], (D, 2 * INNER), D ** -0.5, 0.1875)
    w_pair_out = gaussian(arg_keys[7], (2 * INNER, P_SIZE), (2 * INNER) ** -0.5, 0.5)
    w_up = gaussian(arg_keys[8], (P_SIZE, HID), P_SIZE ** -0.5, 0.5)
    w_down = gaussian(arg_keys[9], (HID, P_SIZE), HID ** -0.5, 0.25)
    return dict(seq_state=seq_state, pair_state=pair_state, w_bias=w_bias, w_qkv=w_qkv, w_gate=w_gate, w_out=w_out, w_seq_pair=w_seq_pair, w_pair_out=w_pair_out, w_up=w_up, w_down=w_down)


EPSILON = 1e-05

def layer_norm(values):
    centred = values - lax.optimization_barrier(jnp.mean(values, axis=-1, keepdims=True))
    variance = lax.optimization_barrier(jnp.mean(centred * centred, axis=-1, keepdims=True))
    return centred * lax.rsqrt(variance + EPSILON)

def reference(seq_state, pair_state, w_bias, w_qkv, w_gate, w_out, w_seq_pair, w_pair_out, w_up, w_down):
    length = seq_state.shape[0]
    model_width = seq_state.shape[1]
    head_count = w_bias.shape[1]
    head_size = model_width // head_count
    channels = pair_state.shape[2]
    blocks = length // RES_DEV
    normed = layer_norm(seq_state.astype(jnp.float32)).astype(jnp.bfloat16)
    queries = jnp.dot(normed, w_qkv[0], preferred_element_type=jnp.float32).astype(jnp.bfloat16)
    keys_all = jnp.dot(normed, w_qkv[1], preferred_element_type=jnp.float32).astype(jnp.bfloat16)
    values_all = jnp.dot(normed, w_qkv[2], preferred_element_type=jnp.float32).astype(jnp.bfloat16)
    gate_values = jax.nn.sigmoid(jnp.dot(normed, w_gate, preferred_element_type=jnp.float32))

    def bias_block(block_rows):
        pair_normed = layer_norm(block_rows.astype(jnp.float32)).astype(jnp.bfloat16)
        flat_norm = pair_normed.reshape(-1, channels)
        return jnp.dot(flat_norm, w_bias, preferred_element_type=jnp.float32).astype(jnp.bfloat16).reshape(block_rows.shape[0], length, head_count)
    bias = lax.map(bias_block, pair_state.reshape(blocks, RES_DEV, length, channels)).reshape(length, length, head_count)
    scale = 1.0 / math.sqrt(head_size)

    def one_head(head_index):
        first_col = head_index * head_size
        query_head = lax.dynamic_slice_in_dim(queries, first_col, head_size, 1)
        key_head = lax.dynamic_slice_in_dim(keys_all, first_col, head_size, 1)
        value_head = lax.dynamic_slice_in_dim(values_all, first_col, head_size, 1)
        head_bias = lax.dynamic_index_in_dim(bias, head_index, 2, keepdims=False)
        scores = jnp.dot(query_head, key_head.T, preferred_element_type=jnp.float32) * scale + head_bias.astype(jnp.float32)
        row_peak = lax.optimization_barrier(jnp.max(scores, axis=-1, keepdims=True))
        weights = jnp.exp(scores - row_peak)
        probs = (weights / lax.optimization_barrier(jnp.sum(weights, axis=-1, keepdims=True))).astype(jnp.bfloat16)
        return jnp.dot(probs, value_head, preferred_element_type=jnp.float32)
    heads_out = lax.map(one_head, jnp.arange(head_count, dtype=jnp.int32))
    mixed_heads = jnp.transpose(heads_out, (1, 0, 2)).reshape(length, model_width)
    attended = (mixed_heads * gate_values).astype(jnp.bfloat16)
    update_seq = jnp.dot(attended, w_out, preferred_element_type=jnp.float32)
    seq_out = (seq_state.astype(jnp.float32) + update_seq).astype(jnp.bfloat16)
    new_normed = layer_norm(seq_out.astype(jnp.float32)).astype(jnp.bfloat16)
    inner_width = w_seq_pair.shape[1] // 2
    projected = lax.optimization_barrier(jnp.dot(new_normed, w_seq_pair, preferred_element_type=jnp.float32).astype(jnp.bfloat16))
    left_side = projected[:, :inner_width].astype(jnp.float32)
    right_side = projected[:, inner_width:].astype(jnp.float32)

    def pair_block(block_items):
        block_rows, left_rows = block_items
        product = left_rows[:, None, :] * right_side[None, :, :]
        difference = left_rows[:, None, :] - right_side[None, :, :]
        features = jnp.concatenate([product, difference], axis=-1).astype(jnp.bfloat16).reshape(-1, 2 * inner_width)
        updated = block_rows.astype(jnp.float32).reshape(-1, channels) + jnp.dot(features, w_pair_out, preferred_element_type=jnp.float32)
        hidden = jax.nn.relu(jnp.dot(layer_norm(updated).astype(jnp.bfloat16), w_up, preferred_element_type=jnp.float32)).astype(jnp.bfloat16)
        result = updated + jnp.dot(hidden, w_down, preferred_element_type=jnp.float32)
        return result.astype(jnp.bfloat16).reshape(block_rows.shape)
    pair_out = lax.map(pair_block, (pair_state.reshape(blocks, RES_DEV, length, channels), left_side.reshape(blocks, RES_DEV, inner_width)))
    return (seq_out, pair_out.reshape(length, length, channels))
```

```python
import functools
import math

import jax
import jax.numpy as jnp
from jax import lax
from jax.experimental import pallas as pl
from jax.experimental.pallas import tpu as pltpu
from jax.sharding import PartitionSpec as P

EPSILON = 1e-05
F32 = jnp.float32
BF16 = jnp.bfloat16
NN = (((1,), (0,)), ((), ()))
NT = (((1,), (1,)), ((), ()))
MESH = pl.DeviceIdType.MESH


def mm(a, b, dims=NN):
    return lax.dot_general(a, b, dims, preferred_element_type=F32)


def layer_norm(values):
    centred = values - jnp.mean(values, axis=-1, keepdims=True)
    variance = jnp.mean(centred * centred, axis=-1, keepdims=True)
    return centred * lax.rsqrt(variance + EPSILON)


def project_kernel(seq_ref, qkv_ref, gate_w_ref, q_ref, kv_ref, gate_ref, normed_ref):
    @pl.when(pl.program_id(0) == 0)
    def _():
        normed_ref[...] = layer_norm(seq_ref[...].astype(F32)).astype(BF16)

    normed = normed_ref[...]
    q_ref[...] = mm(normed, qkv_ref[0]).astype(BF16)
    kv_ref[0] = mm(normed, qkv_ref[1]).astype(BF16)
    kv_ref[1] = mm(normed, qkv_ref[2]).astype(BF16)
    gates = mm(normed, gate_w_ref[...])
    gate_ref[...] = 1.0 / (1.0 + jnp.exp(-gates))


def project(seq_state, w_qkv, w_gate):
    rows, depth = seq_state.shape
    width = w_gate.shape[1]
    tile = min(width, 128)
    return pl.pallas_call(
        project_kernel,
        grid=(width // tile,),
        in_specs=[
            pl.BlockSpec((rows, depth), lambda g: (0, 0)),
            pl.BlockSpec((3, depth, tile), lambda g: (0, 0, g)),
            pl.BlockSpec((depth, tile), lambda g: (0, g)),
        ],
        out_specs=[
            pl.BlockSpec((rows, tile), lambda g: (0, g)),
            pl.BlockSpec((2, rows, tile), lambda g: (0, 0, g)),
            pl.BlockSpec((rows, tile), lambda g: (0, g)),
        ],
        out_shape=[
            jax.ShapeDtypeStruct((rows, width), BF16),
            jax.ShapeDtypeStruct((2, rows, width), BF16),
            jax.ShapeDtypeStruct((rows, width), F32),
        ],
        scratch_shapes=[pltpu.VMEM((rows, depth), BF16)],
        compiler_params=pltpu.CompilerParams(vmem_limit_bytes=60 << 20),
        name="project",
    )(seq_state, w_qkv, w_gate)


def greet(row_count, groups):
    row, col = lax.axis_index("row"), lax.axis_index("col")
    barrier = pltpu.get_barrier_semaphore()
    for d in range(1, row_count):
        pl.semaphore_signal(
            barrier, inc=1, device_id={"row": lax.rem(row + d, row_count)}, device_id_type=MESH
        )
    for d in range(1, groups):
        pl.semaphore_signal(
            barrier, inc=1, device_id={"col": lax.rem(col + d, groups)}, device_id_type=MESH
        )
    pl.semaphore_wait(barrier, row_count + groups - 2)


def split_rows(row_count):
    core = 2 if row_count % 2 == 0 else 1
    near = 2 if (row_count // core) % 2 == 0 else 1
    return row_count // core // near, near, core


def centre_matrix(channels):
    shape = (channels, channels)
    same = lax.broadcasted_iota(jnp.int32, shape, 0) == lax.broadcasted_iota(jnp.int32, shape, 1)
    return jnp.where(same, 1.0, 0.0) - 1.0 / channels


def bias_kernel(
    row_count, groups, pair_ref, w_ref, kv_ref,
    own_ref, kv_all_ref, *rest
):
    received = rest[: groups - 1]
    (send_buf, kv_send, kv_recv, kv_local, bias_send, bias_recv) = rest[groups - 1 :]
    step, steps = pl.program_id(0), pl.num_programs(0)
    step_rows, local_heads, cols = own_ref.shape
    row, col = lax.axis_index("row"), lax.axis_index("col")
    far_n, near_n, core_n = split_rows(row_count)
    far, near, core = row // (near_n * core_n), (row // core_n) % near_n, row % core_n

    def index(f, n, c):
        return (lax.rem(f, far_n) * near_n + lax.rem(n, near_n)) * core_n + lax.rem(c, core_n)

    def kv_copy(slot, source, block, target):
        return pltpu.make_async_remote_copy(
            src_ref=source,
            dst_ref=kv_all_ref.at[block],
            send_sem=kv_send.at[slot],
            recv_sem=kv_recv.at[block],
            device_id={"row": target},
            device_id_type=MESH,
        )

    def far_copies():
        return [
            kv_copy(d - 1, kv_ref, row, index(far + d, near, core)) for d in range(1, far_n)
        ]

    def near_copies(first, last):
        out = []
        for e in range(1, near_n):
            for d in range(first, last):
                block = index(far + d, near, core)
                source = kv_ref if d == 0 else kv_all_ref.at[block]
                slot = far_n - 1 + (e - 1) * far_n + d
                out.append(kv_copy(slot, source, block, index(far, near + e, core)))
        return out

    def core_copies(first_near, last_near, first, last):
        out = []
        for c in range(1, core_n):
            for e in range(first_near, last_near):
                for d in range(first, last):
                    block = index(far + d, near + e, core)
                    source = kv_ref if d == 0 and e == 0 else kv_all_ref.at[block]
                    slot = near_n * far_n - 1 + ((c - 1) * near_n + e) * far_n + d
                    out.append(kv_copy(slot, source, block, index(far, near, core + c)))
        return out

    def wait_block(block):
        kv_copy(0, kv_ref, block, row).wait_recv()

    def local_copy():
        return pltpu.make_async_copy(kv_ref, kv_all_ref.at[row], kv_local)

    def bias_copy(s, at):
        return pltpu.make_async_remote_copy(
            src_ref=send_buf.at[lax.rem(at, 2), s - 1],
            dst_ref=received[s - 1].at[pl.ds(at * step_rows, step_rows)],
            send_sem=bias_send.at[lax.rem(at, 2), s - 1],
            recv_sem=bias_recv.at[at, s - 1],
            device_id={"col": lax.rem(col + s, groups)},
            device_id_type=MESH,
        )

    @pl.when(step == 0)
    def _():
        greet(row_count, groups)
        for copy in far_copies() + near_copies(0, 1) + core_copies(0, 1, 0, 1):
            copy.start()
        local_copy().start()

    @pl.when(step >= 1)
    def _():
        for s in range(1, groups):
            bias_copy(s, step - 1).start()

    @pl.when(step >= 2)
    def _():
        for s in range(1, groups):
            bias_copy(s, step - 2).wait_send()

    slot = lax.rem(step, 2)
    w_rows = jnp.concatenate(
        [w_ref[lax.rem(col + s, groups)].astype(F32) for s in range(groups)], axis=0
    ).astype(BF16)
    centre = centre_matrix(pair_ref.shape[2]).astype(BF16)
    for r in range(step_rows):
        centred = mm(pair_ref[r], centre)
        variance = jnp.mean(centred * centred, axis=-1, keepdims=True)
        normed = (centred * lax.rsqrt(variance + EPSILON)).astype(BF16)
        bias = mm(w_rows, normed, NT).astype(BF16)
        own_ref[r] = bias[:local_heads]
        for s in range(1, groups):
            send_buf[slot, s - 1, r] = bias[s * local_heads : (s + 1) * local_heads]

    @pl.when(step == steps - 1)
    def _():
        for s in range(1, groups):
            bias_copy(s, step).start()
        for d in range(1, far_n):
            wait_block(index(far + d, near, core))
            for copy in near_copies(d, d + 1) + core_copies(0, 1, d, d + 1):
                copy.start()
        for e in range(1, near_n):
            for d in range(far_n):
                wait_block(index(far + d, near + e, core))
                for copy in core_copies(e, e + 1, d, d + 1):
                    copy.start()
        for c in range(1, core_n):
            for e in range(near_n):
                for d in range(far_n):
                    wait_block(index(far + d, near + e, core + c))
        local_copy().wait()
        for copy in far_copies() + near_copies(0, far_n) + core_copies(0, near_n, 0, far_n):
            copy.wait_send()
        for s in range(1, groups):
            @pl.when(step >= 1)
            def _():
                bias_copy(s, step - 1).wait_send()

            bias_copy(s, step).wait_send()

            @pl.loop(0, steps)
            def _(at):
                bias_copy(s, at).wait_recv()


def bias_and_gather(pair_state, w_rows, kv_local, row_count, groups, step_rows):
    rows, cols, channels = pair_state.shape
    local_heads = w_rows.shape[1]
    steps = rows // step_rows
    whole = lambda x: pl.BlockSpec(x.shape, lambda g: (0,) * x.ndim)
    anywhere = pl.BlockSpec(memory_space=pl.ANY)
    part = jax.ShapeDtypeStruct((rows, local_heads, cols), BF16)
    out = pl.pallas_call(
        functools.partial(bias_kernel, row_count, groups),
        grid=(steps,),
        in_specs=[
            pl.BlockSpec((step_rows, cols, channels), lambda g: (g, 0, 0)),
            whole(w_rows),
            anywhere,
        ],
        out_specs=[
            pl.BlockSpec((step_rows, local_heads, cols), lambda g: (g, 0, 0)),
            anywhere,
        ]
        + [anywhere] * (groups - 1),
        out_shape=[part, jax.ShapeDtypeStruct((row_count,) + kv_local.shape, BF16)]
        + [part] * (groups - 1),
        scratch_shapes=[
            pltpu.VMEM((2, max(1, groups - 1), step_rows, local_heads, cols), BF16),
            pltpu.SemaphoreType.DMA((row_count,)),
            pltpu.SemaphoreType.DMA((row_count,)),
            pltpu.SemaphoreType.DMA,
            pltpu.SemaphoreType.DMA((2, max(1, groups - 1))),
            pltpu.SemaphoreType.DMA((steps, max(1, groups - 1))),
        ],
        compiler_params=pltpu.CompilerParams(
            vmem_limit_bytes=60 << 20, collective_id=0, has_side_effects=True
        ),
        name="bias_gather",
    )(pair_state, w_rows, kv_local)
    return out[1], [out[0]] + list(out[2:])


def mix_chunk(head_size, groups, col, q, k_ref, v_ref, gates, bias_refs):
    rows, heads, cols = bias_refs[0].shape
    width = q.shape[1]
    lane_head = lax.broadcasted_iota(jnp.int32, (heads, width), 1) // head_size
    own = (lane_head == lax.broadcasted_iota(jnp.int32, (heads, width), 0)).astype(F32)
    scale = 1.0 / math.sqrt(head_size)
    blocks = cols // k_ref.shape[1]
    queries = (q.astype(F32)[:, None, :] * own[None]).reshape(rows * heads, width).astype(BF16)
    scores, parts = [], []
    for s in range(groups):
        start = lax.rem(col + (groups - s), groups) * blocks
        parts.append(start)
        keys = k_ref[pl.ds(start, blocks)].reshape(cols, width)
        scores.append(
            mm(queries, keys, NT) * scale
            + bias_refs[s][...].astype(F32).reshape(rows * heads, cols)
        )
    peak = functools.reduce(jnp.maximum, [jnp.max(x, axis=-1, keepdims=True) for x in scores])
    weights = [jnp.exp(x - peak) for x in scores]
    inverse = 1.0 / sum(jnp.sum(x, axis=-1, keepdims=True) for x in weights)
    mixed = sum(
        mm((x * inverse).astype(BF16), v_ref[pl.ds(start, blocks)].reshape(cols, width))
        for x, start in zip(weights, parts)
    )
    mixed = jnp.sum(mixed.reshape(rows, heads, width) * own[None], axis=1)
    return (mixed * gates).astype(BF16)


def attend_kernel(
    head_size, row_count, groups, q_ref, k_ref, v_ref, gate_ref, seq_ref, w_out_ref,
    w_sides_ref, *rest
):
    bias_refs = rest[:groups]
    (seq_out_ref, left_ref, right_all_ref) = rest[groups : groups + 3]
    (attended, projected, mix_send, mix_recv, side_send, side_recv, side_local) = rest[groups + 3 :]
    step, steps = pl.program_id(0), pl.num_programs(0)
    chunk, width = q_ref.shape
    rows, depth = seq_ref.shape
    row, col = lax.axis_index("row"), lax.axis_index("col")
    blocks = right_all_ref.shape[0]

    def mix_copy(s, at):
        here = pl.ds(at * chunk, chunk)
        return pltpu.make_async_remote_copy(
            src_ref=attended.at[0, here],
            dst_ref=attended.at[s, here],
            send_sem=mix_send.at[at, s],
            recv_sem=mix_recv.at[at, s],
            device_id={"col": lax.rem(col + s, groups)},
            device_id_type=MESH,
        )

    def side_copy(d):
        return pltpu.make_async_remote_copy(
            src_ref=projected,
            dst_ref=right_all_ref.at[lax.rem(row, blocks)],
            send_sem=side_send.at[d],
            recv_sem=side_recv.at[lax.rem(row, blocks)],
            device_id={"row": lax.rem(row + d, row_count)},
            device_id_type=MESH,
        )

    def side_wait(block):
        pltpu.make_async_remote_copy(
            src_ref=projected,
            dst_ref=right_all_ref.at[block],
            send_sem=side_send.at[0],
            recv_sem=side_recv.at[block],
            device_id={"row": row},
            device_id_type=MESH,
        ).wait_recv()

    @pl.when(step == 0)
    def _():
        greet(row_count, groups)

    @pl.when(step >= 1)
    def _():
        for s in range(1, groups):
            mix_copy(s, step - 1).start()

    attended[0, pl.ds(step * chunk, chunk)] = mix_chunk(
        head_size, groups, col, q_ref[...], k_ref, v_ref, gate_ref[...], bias_refs
    )

    @pl.when(step == steps - 1)
    def _():
        total = seq_ref[...].astype(F32)
        for s in range(1, groups):
            mix_copy(s, step).start()
        start = pl.multiple_of(col * width, width)
        update = mm(attended[0], w_out_ref[pl.ds(start, width), :])
        for s in range(1, groups):
            for at in range(steps_static(rows, chunk)):
                mix_copy(s, at).wait_recv()
            source = lax.rem(col + (groups - s), groups)
            start = pl.multiple_of(source * width, width)
            update += mm(attended[s], w_out_ref[pl.ds(start, width), :])
        seq_out = (total + update).astype(BF16)
        seq_out_ref[...] = seq_out
        normed = layer_norm(seq_out.astype(F32)).astype(BF16)
        sides = mm(normed, w_sides_ref[...])
        inner = sides.shape[1] // 2
        lanes = lax.broadcasted_iota(jnp.int32, sides.shape, 1)
        projected[...] = jnp.where(lanes < inner, pltpu.roll(sides, inner, 1), sides).astype(BF16)
        mine = row // blocks == col

        @pl.when(mine)
        def _():
            for d in range(1, row_count):
                side_copy(d).start()
            pltpu.make_async_copy(
                projected, right_all_ref.at[lax.rem(row, blocks)], side_local
            ).start()

        left_ref[...] = jnp.where(lanes < inner, sides.astype(BF16).astype(F32), 1.0)

        for b in range(blocks):
            @pl.when(col * blocks + b != row)
            def _():
                side_wait(b)

        @pl.when(mine)
        def _():
            pltpu.make_async_copy(
                projected, right_all_ref.at[lax.rem(row, blocks)], side_local
            ).wait()
            for d in range(1, row_count):
                side_copy(d).wait_send()

        for s in range(1, groups):
            for at in range(steps_static(rows, chunk)):
                mix_copy(s, at).wait_send()


def steps_static(rows, chunk):
    return rows // chunk


def attend(queries, kv_all, gates, biases, seq_state, w_out, w_seq_pair, head_size, row_count, chunk):
    rows, depth = seq_state.shape
    groups = len(biases)
    heads, cols = biases[0].shape[1:]
    width = queries.shape[1]
    inner = w_seq_pair.shape[1] // 2
    blocks = cols // rows
    whole = lambda x: pl.BlockSpec(x.shape, lambda g: (0,) * x.ndim, pipeline_mode=pl.Buffered(1))
    side = lambda i: pl.BlockSpec(
        (row_count, None, rows, width), lambda g: (0, i, 0, 0), pipeline_mode=pl.Buffered(1)
    )
    steps = rows // chunk
    fixed = lambda shape: pl.BlockSpec(shape, lambda g: (0,) * len(shape))
    return pl.pallas_call(
        functools.partial(attend_kernel, head_size, row_count, groups),
        grid=(steps,),
        in_specs=[
            pl.BlockSpec((chunk, width), lambda g: (g, 0)),
            side(0),
            side(1),
            pl.BlockSpec((chunk, width), lambda g: (g, 0)),
            whole(seq_state),
            whole(w_out),
            whole(w_seq_pair),
        ]
        + [pl.BlockSpec((chunk, heads, cols), lambda g: (g, 0, 0))] * groups,
        out_specs=[
            fixed((rows, depth)),
            fixed((rows, 2 * inner)),
            pl.BlockSpec(memory_space=pl.ANY),
        ],
        out_shape=[
            jax.ShapeDtypeStruct((rows, depth), BF16),
            jax.ShapeDtypeStruct((rows, 2 * inner), F32),
            jax.ShapeDtypeStruct((blocks, rows, 2 * inner), BF16),
        ],
        scratch_shapes=[
            pltpu.VMEM((groups, rows, width), BF16),
            pltpu.VMEM((rows, 2 * inner), BF16),
            pltpu.SemaphoreType.DMA((steps, groups)),
            pltpu.SemaphoreType.DMA((steps, groups)),
            pltpu.SemaphoreType.DMA((row_count,)),
            pltpu.SemaphoreType.DMA((blocks,)),
            pltpu.SemaphoreType.DMA,
        ],
        compiler_params=pltpu.CompilerParams(
            vmem_limit_bytes=60 << 20, collective_id=1, has_side_effects=True
        ),
        name="attend",
    )(queries, kv_all, kv_all, gates, seq_state, w_out, w_seq_pair, *biases)


def pair_kernel(
    left_ref, pair_ref, right_ref, w_pair_ref, up_ref, down_ref, out_ref,
    w_pair_t, up_t, down_t, right_t, left_t, updated_buf, centred_buf, scale_buf, hidden_buf,
):
    step_rows, cols, channels = pair_ref.shape
    inner = w_pair_ref.shape[0] // 2
    base = pl.program_id(0) * step_rows

    @pl.when(pl.program_id(0) == 0)
    def _():
        w_pair_t[...] = w_pair_ref[...].T
        up_t[...] = up_ref[...].T
        down_t[...] = down_ref[...].T
        right_t[...] = right_ref[...].T[:inner]
        left = left_ref[:, :inner]
        rows = left.shape[0]
        padded = jnp.concatenate([left, jnp.zeros((left_t.shape[1] - rows, inner), F32)], axis=0)
        left_t[...] = padded.T

    lefts = pltpu.roll(left_t[...], lax.rem(left_t.shape[1] - base, left_t.shape[1]), 1)
    right = right_t[...]

    def features(r):
        slot = r % 3
        left = lefts[:, r : r + 1].astype(BF16)
        sides = jnp.concatenate([left * right, left - right], axis=0)
        updated = pair_ref[r].T.astype(F32) + mm(w_pair_t[...], sides)
        centred = updated - jnp.mean(updated, axis=0, keepdims=True)
        variance = jnp.mean(centred * centred, axis=0, keepdims=True)
        updated_buf[slot] = updated
        centred_buf[r % 2] = centred.astype(BF16)
        scale_buf[slot] = lax.rsqrt(variance + EPSILON)

    def expand(r):
        hidden_buf[r % 2] = jnp.maximum(mm(up_t[...], centred_buf[r % 2]).astype(BF16), 0.0)

    def contract(r):
        slot = r % 3
        change = mm(down_t[...], hidden_buf[r % 2]) * scale_buf[slot]
        out_ref[r] = (updated_buf[slot] + change).astype(BF16).T

    for t in range(step_rows + 2):
        if t < step_rows:
            features(t)
        if 0 <= t - 1 < step_rows:
            expand(t - 1)
        if t >= 2:
            contract(t - 2)


def pair_update(pair_state, left, right, w_pair_out, w_up, w_down, step_rows):
    rows, cols, channels = pair_state.shape
    whole = lambda x: pl.BlockSpec(x.shape, lambda g: (0,) * x.ndim)
    return pl.pallas_call(
        pair_kernel,
        grid=(rows // step_rows,),
        in_specs=[
            whole(left),
            pl.BlockSpec((step_rows, cols, channels), lambda g: (g, 0, 0)),
            whole(right),
            whole(w_pair_out),
            whole(w_up),
            whole(w_down),
        ],
        out_specs=pl.BlockSpec((step_rows, cols, channels), lambda g: (g, 0, 0)),
        out_shape=jax.ShapeDtypeStruct(pair_state.shape, BF16),
        scratch_shapes=[
            pltpu.VMEM(w_pair_out.shape[::-1], BF16),
            pltpu.VMEM(w_up.shape[::-1], BF16),
            pltpu.VMEM(w_down.shape[::-1], BF16),
            pltpu.VMEM((right.shape[1] // 2, cols), BF16),
            pltpu.VMEM((right.shape[1] // 2, max(128, rows)), F32),
            pltpu.VMEM((3, channels, cols), F32),
            pltpu.VMEM((2, channels, cols), BF16),
            pltpu.VMEM((3, 1, cols), F32),
            pltpu.VMEM((2, w_up.shape[1], cols), BF16),
        ],
        compiler_params=pltpu.CompilerParams(vmem_limit_bytes=60 << 20),
        name="pair_update",
    )(left, pair_state, right, w_pair_out, w_up, w_down)


def body(row_count, groups, seq_state, pair_state, w_bias, w_qkv, w_gate, w_out, w_seq_pair, w_pair_out, w_up, w_down):
    rows_here, model_width = seq_state.shape
    cols_here, channels = pair_state.shape[1:]
    head_count = w_bias.shape[1]
    local_width = w_gate.shape[1]
    head_size = model_width // head_count
    local_heads = local_width // head_size
    queries, kv_local, gates = project(seq_state, w_qkv, w_gate)
    w_rows = w_bias.T.reshape(groups, local_heads, channels)
    kv_all, biases = bias_and_gather(
        pair_state, w_rows, kv_local, row_count, groups, math.gcd(rows_here, 8)
    )
    seq_out, left, right = attend(
        queries, kv_all, gates, biases, seq_state, w_out, w_seq_pair,
        head_size, row_count, math.gcd(rows_here, 32),
    )
    right = right.reshape(cols_here, right.shape[-1])
    pair_out = pair_update(pair_state, left, right, w_pair_out, w_up, w_down, math.gcd(rows_here, 16))
    return seq_out, pair_out


def solution(mesh):
    return jax.shard_map(
        functools.partial(body, mesh.shape["row"], mesh.shape["col"]),
        mesh=mesh,
        in_specs=(
            P("row", None),
            P("row", "col", None),
            P(),
            P(None, None, "col"),
            P(None, "col"),
            P(),
            P(),
            P(),
            P(),
            P(),
        ),
        out_specs=(P("row", None), P("row", "col", None)),
        check_vma=False,
    )
```
